32 devices in a mesh: dx: 2 (over x), dy: 16 (over z, y, core).
Axes of the slice: x: 2, y: 2, z: 4, core: 2. Of those that a mesh axis runs over, the one named last changes fastest.
Arguments:
- seg_mid: float32 [2, 16, 3, 4096], P('dx', 'dy'), may hold values from 0 to 1
- seg_line: float32 [2, 16, 3, 4096], P('dx', 'dy'), may hold values from -0.3 to 0.3
- seg_burgers: float32 [2, 16, 3, 4096], P('dx', 'dy'), may hold values from -5 to 5
- seg_cell: int32 [2, 16, 4096], P('dx', 'dy'), may hold values from 0 to 71, as said below
- seg_node: int32 [2, 16, 2, 4096], P('dx', 'dy'), may hold values from 0 to 4607, as said below
- ghost_list: int32 [2, 16, 8, 2], P('dx', 'dy'), may hold values from 0 to 31
- ghost_count: int32 [2, 16, 8], P('dx', 'dy'), may hold values from 1 to 2
- pair_list: int32 [2, 16, 32, 12], P('dx', 'dy'), may hold values from 0 to 47, as said below
- pair_count: int32 [2, 16, 32], P('dx', 'dy'), may hold values from 1 to 12
Outputs:
- node_force: float32 [2, 16, 3, 512], P('dx', 'dy')
- cell_moments: float32 [315, 256], P(None, ('dx', 'dy'))
The draws below stay inside these ranges and needn't reach their ends.
Inputs may be any that keep to these rules, and one draw needn't show every extreme that they name: `seg_node`: each entry is d * 512 + m with m a node of the domain at offset (a, b) from the segment's domain, d = 3 (a + 1) + (b + 1), a and b in -1, 0, 1; d = 4 is the domain itself. `seg_cell`: each entry is d * 8 + c with c a cell owned by the domain at offset (a, b) from the segment's domain, d = 3 (a + 1) + (b + 1), a and b in -1, 0, 1; d = 4 is the domain itself. `pair_list`: the entries of one tile's list are distinct.
All inputs are finite; a program needn't handle non-finite values.
Results may differ from the reference program's by a relative error of at most 0.0003.
Values sent between devices are 32-bit elements; how exact they have to be, the bound alone decides.
A program may use at most 64 MiB of HBM per device.

```python
import jax
import jax.numpy as jnp
import numpy as np
from jax import lax

TILE = 128
TILES = 32
GHOST = 2
NP = 12
NODE_DEV = 512
CELL_DEV = 8
COMPONENTS = 315
SEG_DEV = 4096
POOL = 48
CELLS = 256
N_DX = 2
N_DY = 16


def draw_seg_node(key, part):
    stay_key, other_key, local_key = jax.random.split(jax.random.fold_in(key, 11), 3)
    shape = (N_DX, N_DY, 2, TILES * TILE)
    staying = jax.random.randint(stay_key, shape, 0, 2)
    elsewhere = jax.random.randint(other_key, shape, 0, 8)
    elsewhere = elsewhere + (elsewhere >= 4).astype(jnp.int32)
    direction = jnp.where(staying == 1, 4, elsewhere)
    local_node = jax.random.randint(local_key, shape, 0, NODE_DEV)
    return (direction * NODE_DEV + local_node).astype(jnp.int32)


def draw_seg_cell(key, part):
    stay_key, other_key, local_key = jax.random.split(jax.random.fold_in(key, 37), 3)
    shape = (N_DX, N_DY, TILES * TILE)
    staying = jax.random.randint(stay_key, shape, 0, 2)
    elsewhere = jax.random.randint(other_key, shape, 0, 8)
    elsewhere = elsewhere + (elsewhere >= 4).astype(jnp.int32)
    direction = jnp.where(staying == 1, 4, elsewhere)
    local_cell = jax.random.randint(local_key, shape, 0, CELL_DEV)
    return (direction * CELL_DEV + local_cell).astype(jnp.int32)


def draw_pair_list(key, part):
    pool_size = TILES + 8 * GHOST
    scores = jax.random.randint(jax.random.fold_in(key, 23), (N_DX, N_DY, TILES, pool_size), 0, 1 << 20)
    scores = scores * pool_size + jnp.arange(pool_size, dtype=jnp.int32)
    ranking = jnp.argsort(scores, axis=-1)
    return ranking[..., :NP].astype(jnp.int32)


def touch_ends(result, rng, smallest, top_value):
    shape = result.shape
    index_at = [jax.random.randint(jax.random.fold_in(rng, axis), (), 0, shape[axis]) for axis in range(len(shape))]
    result = result.at[tuple(index_at)].set(smallest)
    longest = shape.index(max(shape))
    index_at[longest] = (index_at[longest] + 1) % shape[longest]
    return result.at[tuple(index_at)].set(top_value)


def block_scale(key, dims, cuts, least, largest):
    factor_of, own = 1.0, jax.random.fold_in(key, 6)
    for dim, blocks in cuts:
        steps = jnp.exp(jax.random.uniform(jax.random.fold_in(own, dim), (blocks,), jnp.float32, least / len(cuts), largest / len(cuts)))
        factor_of = factor_of * jnp.repeat(steps, dims[dim] // blocks).reshape([-1 if axis == dim else 1 for axis in range(len(dims))])
    return factor_of


def normal_values(key, extent, width, bound, pieces=(), kind=jnp.bfloat16):
    values = width * jax.random.normal(key, extent, jnp.float32)
    if pieces:
        values = values * block_scale(key, extent, pieces, -0.22, 0.18)
    return jnp.clip(values, -bound, bound).astype(kind)


def setup_inputs(seed: int = 0) -> dict:
    streams_of = jax.random.split(jax.random.key(seed), 10)
    seg_mid = jnp.clip(1.0 * jax.random.uniform(streams_of[0], (N_DX, N_DY, 3, SEG_DEV), jnp.float32) ** block_scale(streams_of[0], (N_DX, N_DY, 3, SEG_DEV), ((0, 2), (1, 16)), -0.2, 0.2), 0.0, 1.0)
    seg_line = normal_values(streams_of[1], (N_DX, N_DY, 3, SEG_DEV), 0.05, 0.3, ((0, 2), (1, 16)), jnp.float32)
    seg_burgers = normal_values(streams_of[2], (N_DX, N_DY, 3, SEG_DEV), 1.0, 5.0, ((0, 2), (1, 16)), jnp.float32)
    seg_cell = draw_seg_cell(jax.random.fold_in(streams_of[9], 71), 0)
    seg_node = draw_seg_node(jax.random.fold_in(streams_of[9], 71), 0)
    ghost_list = touch_ends(jax.random.randint(streams_of[5], (N_DX, N_DY, 8, GHOST), 0, TILES), jax.random.fold_in(streams_of[5], 1), 0, TILES - 1).astype(jnp.int32)
    ghost_count = touch_ends(jax.random.randint(streams_of[6], (N_DX, N_DY, 8), 1, GHOST + 1), jax.random.fold_in(streams_of[6], 1), 1, GHOST).astype(jnp.int32)
    pair_list = draw_pair_list(jax.random.fold_in(streams_of[9], 71), 0)
    pair_count = touch_ends(jax.random.randint(streams_of[8], (N_DX, N_DY, TILES), 1, NP + 1), jax.random.fold_in(streams_of[8], 1), 1, NP).astype(jnp.int32)
    return dict(seg_mid=seg_mid, seg_line=seg_line, seg_burgers=seg_burgers, seg_cell=seg_cell, seg_node=seg_node, ghost_list=ghost_list, ghost_count=ghost_count, pair_list=pair_list, pair_count=pair_count)


core_radius = 0.1
shear_scale = 0.25
neighbour_offsets = ((-1, -1), (-1, 0), (-1, 1), (0, -1), (0, 1), (1, -1), (1, 0), (1, 1))

def exponent_table():
    exponent_rows = []
    for degree in range(5):
        for first_power in range(degree, -1, -1):
            for second in range(degree - first_power, -1, -1):
                exponent_rows.append((first_power, second, degree - first_power - second))
    return np.array(exponent_rows, dtype=np.int32)

def moment_terms(midpoint, line_vector, burgers):
    scaled = 2.0 * (midpoint - 0.5)
    powers = jnp.stack([jnp.ones_like(scaled), scaled, scaled * scaled, scaled ** 3, scaled ** 4], axis=1)
    exponents = exponent_table()
    monomial = powers[0, exponents[:, 0]] * powers[1, exponents[:, 1]] * powers[2, exponents[:, 2]]
    products = (burgers[:, None, :] * line_vector[None, :, :]).reshape(9, -1)
    return (products[:, None, :] * monomial[None, :, :]).reshape(9 * monomial.shape[0], -1)

def pair_stress(field_tiles, source_tiles, valid_weight):
    separation = [field_tiles[component][:, :, None] - source_tiles[component][:, None, :] for component in range(3)]
    line_source = source_tiles[3:6]
    burgers_source = source_tiles[6:9]
    cross_source = [burgers_source[1] * line_source[2] - burgers_source[2] * line_source[1], burgers_source[2] * line_source[0] - burgers_source[0] * line_source[2], burgers_source[0] * line_source[1] - burgers_source[1] * line_source[0]]
    cross_source = [entry_value[:, None, :] for entry_value in cross_source]
    radius_sq = separation[0] ** 2 + separation[1] ** 2 + separation[2] ** 2 + core_radius ** 2
    inverse = 1.0 / jnp.sqrt(radius_sq)
    weight = shear_scale * valid_weight[:, None, None] * inverse / radius_sq
    projection = separation[0] * cross_source[0] + separation[1] * cross_source[1] + separation[2] * cross_source[2]
    diagonal_term = projection * (1.0 + 1.5 * core_radius ** 2 / radius_sq)
    entries = []
    for first_axis, second_axis in ((0, 0), (1, 1), (2, 2), (0, 1), (0, 2), (1, 2)):
        entry_value = separation[first_axis] * cross_source[second_axis] + separation[second_axis] * cross_source[first_axis] - 3.0 * projection * separation[first_axis] * separation[second_axis] / radius_sq
        if first_axis == second_axis:
            entry_value = entry_value + diagonal_term
        entries.append(lax.optimization_barrier(jnp.sum(weight * entry_value, axis=2)))
    return jnp.stack(entries)

def segment_force(stress, own_columns):
    line_vector = own_columns[3:6]
    burgers = own_columns[6:9]
    traction = [stress[0] * burgers[0] + stress[3] * burgers[1] + stress[4] * burgers[2], stress[3] * burgers[0] + stress[1] * burgers[1] + stress[5] * burgers[2], stress[4] * burgers[0] + stress[5] * burgers[1] + stress[2] * burgers[2]]
    return jnp.stack([traction[1] * line_vector[2] - traction[2] * line_vector[1], traction[2] * line_vector[0] - traction[0] * line_vector[2], traction[0] * line_vector[1] - traction[1] * line_vector[0]])

def reference(seg_mid, seg_line, seg_burgers, seg_cell, seg_node, ghost_list, ghost_count, pair_list, pair_count):
    width_x = seg_mid.shape[0]
    width_y = seg_mid.shape[1]
    seg_data = jnp.concatenate([seg_mid, seg_line, seg_burgers], axis=2)
    own_tiles = seg_data.reshape(width_x, width_y, 9, TILES, TILE).transpose(0, 1, 3, 2, 4)
    packets = jax.vmap(jax.vmap(lambda tile_set, chosen: tile_set[chosen]))(own_tiles, ghost_list)
    slot_valid = (jnp.arange(GHOST, dtype=jnp.int32)[None, None, None, :] < ghost_count[..., None]).astype(jnp.float32)
    packets = packets * slot_valid[..., None, None]
    groups = []
    for group_index in range(8):
        first_shift, second_shift = neighbour_offsets[group_index]
        incoming = jnp.roll(packets[:, :, 7 - group_index], shift=(-first_shift, -second_shift), axis=(0, 1))
        offset_rows = jnp.array([first_shift, second_shift, 0, 0, 0, 0, 0, 0, 0], jnp.float32)
        groups.append(incoming + offset_rows[None, None, None, :, None])
    source_pool = jnp.concatenate([own_tiles] + groups, axis=2)
    total_domains = width_x * width_y

    def domain_partial(inputs):
        pool_dev, own_dev, pairs_dev, limit_dev, ends_dev = inputs
        own_columns = own_dev.transpose(1, 0, 2)

        def add_slot(stress_total, slot_index):
            source_tiles = pool_dev[pairs_dev[:, slot_index]].transpose(1, 0, 2)
            valid_weight = (slot_index < limit_dev).astype(jnp.float32)
            return (stress_total + pair_stress(own_columns, source_tiles, valid_weight), None)
        stress_total, unused = lax.scan(add_slot, jnp.zeros((6, TILES, TILE), jnp.float32), jnp.arange(NP, dtype=jnp.int32))
        force = segment_force(stress_total, own_columns).reshape(3, TILES * TILE)
        halves = 0.5 * force.T
        partial_value = jax.ops.segment_sum(jnp.concatenate([halves, halves], axis=0), jnp.concatenate([ends_dev[0], ends_dev[1]]).astype(jnp.int32), num_segments=9 * NODE_DEV)
        return partial_value.reshape(9, NODE_DEV, 3).transpose(0, 2, 1)
    partials = lax.map(domain_partial, (source_pool.reshape(total_domains, POOL, 9, TILE), own_tiles.reshape(total_domains, TILES, 9, TILE), pair_list.reshape(total_domains, TILES, NP), pair_count.reshape(total_domains, TILES), seg_node.reshape(total_domains, 2, TILES * TILE)))
    partials = partials.reshape(width_x, width_y, 9, 3, NODE_DEV)
    node_force = jnp.zeros((width_x, width_y, 3, NODE_DEV), jnp.float32)
    for direction in range(9):
        node_force = node_force + jnp.roll(partials[:, :, direction], shift=(direction // 3 - 1, direction % 3 - 1), axis=(0, 1))

    def cell_partial(inputs):
        mid_dev, line_dev, burgers_dev, cell_dev = inputs
        terms = moment_terms(mid_dev, line_dev, burgers_dev)
        return jax.ops.segment_sum(terms.T, cell_dev.astype(jnp.int32), num_segments=9 * CELL_DEV)
    cell_parts = lax.map(cell_partial, (seg_mid.reshape(total_domains, 3, TILES * TILE), seg_line.reshape(total_domains, 3, TILES * TILE), seg_burgers.reshape(total_domains, 3, TILES * TILE), seg_cell.reshape(total_domains, TILES * TILE)))
    cell_parts = cell_parts.reshape(width_x, width_y, 9, CELL_DEV, COMPONENTS)
    cell_grid = jnp.zeros((width_x, width_y, CELL_DEV, COMPONENTS), jnp.float32)
    for direction in range(9):
        cell_grid = cell_grid + jnp.roll(cell_parts[:, :, direction], shift=(direction // 3 - 1, direction % 3 - 1), axis=(0, 1))
    return (node_force, cell_grid.reshape(CELLS, COMPONENTS).T)
```

```python
import functools

import jax
import jax.numpy as jnp
from jax import lax
from jax.experimental import pallas as pl
from jax.experimental.pallas import tpu as pltpu
from jax.sharding import PartitionSpec as P

TILE = 128
GROUP = 8
MONO_ROWS = 40
NODE_ROWS = 16

core_radius = 0.1
shear_scale = 0.25
neighbour_offsets = ((-1, -1), (-1, 0), (-1, 1), (0, -1), (0, 1), (1, -1), (1, 0), (1, 1))


def passed_along(block, axis, distance):
    devices = range(lax.axis_size(axis))
    route = [((i - distance) % len(devices), i) for i in devices]
    return lax.ppermute(block, axis, route)


def exponent_rows():
    rows = []
    for degree in range(5):
        for first in range(degree, -1, -1):
            for second in range(degree - first, -1, -1):
                rows.append((first, second, degree - first - second))
    return rows


def split_two(value):
    high = value.astype(jnp.bfloat16)
    low = (value - high.astype(jnp.float32)).astype(jnp.bfloat16)
    return high, low


def dot_lanes(left, right):
    return lax.dot_general(
        left, right, (((1,), (1,)), ((), ())), preferred_element_type=jnp.float32
    )


def cell_partial(mid_ref, line_ref, burgers_ref, cell_ref, mono_ref, chunk):
    segments = mid_ref.shape[1]
    mono_ref[...] = jnp.zeros_like(mono_ref)
    total = None
    for start in range(0, segments, chunk):
        cols = pl.ds(start, chunk)
        powers = []
        for axis in range(3):
            scaled = 2.0 * (mid_ref[axis : axis + 1, cols] - 0.5)
            square = scaled * scaled
            powers.append((None, scaled, square, square * scaled, square * square))
        for row, exps in enumerate(exponent_rows()):
            value = None
            for axis in range(3):
                if exps[axis]:
                    factor = powers[axis][exps[axis]]
                    value = factor if value is None else value * factor
            if value is None:
                value = jnp.ones((1, chunk), jnp.float32)
            mono_ref[row : row + 1, :] = value
        mono = mono_ref[...]
        highs, lows = [], []
        for beta in range(3):
            b = burgers_ref[beta : beta + 1, cols]
            for gamma in range(3):
                high, low = split_two(mono * (b * line_ref[gamma : gamma + 1, cols]))
                highs.append(high)
                lows.append(low)
        rows = lax.broadcasted_iota(jnp.int32, (TILE, chunk), 0)
        member = jnp.where(rows == cell_ref[0:1, cols], 1.0, 0.0).astype(jnp.bfloat16)
        part = dot_lanes(jnp.concatenate(highs, axis=0), member) + dot_lanes(
            jnp.concatenate(lows, axis=0), member
        )
        total = part if total is None else total + part
    return total


def cells_kernel(mid_ref, line_ref, burgers_ref, cell_ref, out_ref, mono_ref):
    total = cell_partial(mid_ref, line_ref, burgers_ref, cell_ref, mono_ref, mono_ref.shape[1])
    pad = out_ref.shape[1] - total.shape[0]
    total = jnp.concatenate([total, jnp.zeros((pad, TILE), jnp.float32)], axis=0)
    out_ref[...] = total.T[: out_ref.shape[0]]


def spread(mid, line, burgers, source_ref, index):
    g = [
        burgers[1] * line[2] - burgers[2] * line[1],
        burgers[2] * line[0] - burgers[0] * line[2],
        burgers[0] * line[1] - burgers[1] * line[0],
    ]
    rows = list(mid) + [shear_scale * value for value in g]
    rows = rows + [jnp.zeros((2, TILE), jnp.float32)]
    columns = jnp.concatenate(rows, axis=0).T
    for q in range(6):
        source_ref[index, q] = jnp.broadcast_to(columns[:, q : q + 1], (TILE, TILE))


def rows_of(ref, cols):
    return [ref[axis : axis + 1, cols] for axis in range(3)]


def force_kernel(
    list_ref, count_ref, mid_ref, line_ref, burgers_ref, node_ref, ghost_ref, out_ref,
    source_ref, force_ref,
):
    own_count = mid_ref.shape[1] // TILE
    ghost_slots = ghost_ref.shape[0] // 8

    def spread_own(tile, carry):
        cols = pl.ds(pl.multiple_of(tile * TILE, TILE), TILE)
        spread(
            rows_of(mid_ref, cols), rows_of(line_ref, cols), rows_of(burgers_ref, cols),
            source_ref, tile,
        )
        return carry

    lax.fori_loop(0, own_count, spread_own, 0, unroll=2)

    def spread_ghost(slot, carry):
        q = slot // ghost_slots
        d = q + jnp.where(q >= 4, 1, 0)
        shift = ((d // 3 - 1).astype(jnp.float32), (d % 3 - 1).astype(jnp.float32), 0.0)
        rows = [ghost_ref[slot, r : r + 1, :] for r in range(9)]
        mid = [rows[axis] + shift[axis] for axis in range(3)]
        spread(mid, rows[3:6], rows[6:9], source_ref, own_count + slot)
        return carry

    lax.fori_loop(0, 8 * ghost_slots, spread_ghost, 0, unroll=2)

    def one_tile(tile, carry):
        cols = pl.ds(pl.multiple_of(tile * TILE, TILE), TILE)
        x = [jnp.broadcast_to(row, (GROUP, TILE)) for row in rows_of(mid_ref, cols)]

        def one_slot(slot, sums):
            source = list_ref[tile, slot]
            sums = list(sums)
            for k in range(TILE // GROUP):
                part = pl.ds(k * GROUP, GROUP)
                R = [x[m] - source_ref[source, m, part, :] for m in range(3)]
                g = [source_ref[source, 3 + m, part, :] for m in range(3)]
                r2 = (R[0] * R[0] + core_radius**2) + (R[1] * R[1] + R[2] * R[2])
                inverse = lax.rsqrt(r2)
                inverse2 = inverse * inverse
                weight = inverse2 * inverse
                p = R[0] * g[0] + R[1] * g[1] + R[2] * g[2]
                h = p * (1.5 * inverse2)
                a = [g[m] - h * R[m] for m in range(3)]
                A = [weight * R[m] for m in range(3)]
                sums[0] = sums[0] + A[0] * a[0]
                sums[1] = sums[1] + A[1] * a[1]
                sums[2] = sums[2] + A[2] * a[2]
                sums[3] = sums[3] + (A[0] * a[1] + A[1] * a[0])
                sums[4] = sums[4] + (A[0] * a[2] + A[2] * a[0])
                sums[5] = sums[5] + (A[1] * a[2] + A[2] * a[1])
                sums[6] = sums[6] + weight * p
            return tuple(sums)

        zero = jnp.zeros((GROUP, TILE), jnp.float32)
        sums = lax.fori_loop(0, count_ref[tile], one_slot, (zero,) * 7)
        s = [jnp.sum(value, axis=0, keepdims=True) for value in sums]
        diagonal = s[0] + s[1] + s[2] + 1.5 * s[6]
        xx, yy, zz = [2.0 * s[m] + diagonal for m in range(3)]
        xy, xz, yz = s[3:6]
        b = rows_of(burgers_ref, cols)
        l = rows_of(line_ref, cols)
        t = [
            xx * b[0] + xy * b[1] + xz * b[2],
            xy * b[0] + yy * b[1] + yz * b[2],
            xz * b[0] + yz * b[1] + zz * b[2],
        ]
        force_ref[0:1, cols] = 0.5 * (t[1] * l[2] - t[2] * l[1])
        force_ref[1:2, cols] = 0.5 * (t[2] * l[0] - t[0] * l[2])
        force_ref[2:3, cols] = 0.5 * (t[0] * l[1] - t[1] * l[0])
        return carry

    lax.fori_loop(0, own_count, one_tile, 0)

    directions = out_ref.shape[0]
    chunk = 8 * TILE
    quads = NODE_ROWS // 4

    def nodes(step, total):
        cols = pl.ds(pl.multiple_of(step * chunk, chunk), chunk)
        rows = [jnp.broadcast_to(force_ref[m : m + 1, cols], (4, chunk)) for m in range(3)]
        rows = jnp.concatenate(rows + [jnp.zeros((4, chunk), jnp.float32)], axis=0)
        high = rows.astype(jnp.bfloat16).astype(jnp.float32)
        low = rows - high
        place = lax.broadcasted_iota(jnp.int32, (NODE_ROWS, chunk), 0) % quads
        lanes = lax.broadcasted_iota(jnp.int32, (TILE, chunk), 0)
        for end in range(2):
            node = node_ref[end : end + 1, cols]
            member = jnp.where(lanes == node % TILE, 1.0, 0.0).astype(jnp.bfloat16)
            block = node // TILE - place
            left = []
            for value in (high, low):
                for d in range(directions):
                    chosen = jnp.where(block == d * quads, value, 0.0)
                    left.append(chosen.astype(jnp.bfloat16))
            total = total + dot_lanes(jnp.concatenate(left, axis=0), member)
        return total

    total = lax.fori_loop(
        0, mid_ref.shape[1] // chunk, nodes,
        jnp.zeros((2 * directions * NODE_ROWS, TILE), jnp.float32),
    )
    half = directions * NODE_ROWS
    out_ref[...] = (total[:half] + total[half:]).reshape(out_ref.shape)


def vmem():
    return pl.BlockSpec(memory_space=pltpu.VMEM)


def smem():
    return pl.BlockSpec(memory_space=pltpu.SMEM)


def cells_call(mid, line, burgers, cell, cell_rows):
    return pl.pallas_call(
        cells_kernel,
        out_shape=jax.ShapeDtypeStruct((cell_rows, 3 * TILE), jnp.float32),
        in_specs=[vmem()] * 4,
        out_specs=vmem(),
        scratch_shapes=[pltpu.VMEM((MONO_ROWS, 4 * TILE), jnp.float32)],
        compiler_params=pltpu.CompilerParams(vmem_limit_bytes=16 << 20),
        cost_estimate=pl.CostEstimate(flops=10**9, bytes_accessed=10**6, transcendentals=0),
    )(mid, line, burgers, cell)


def force_call(pairs, counts, mid, line, burgers, node, ghosts):
    pool = mid.shape[1] // TILE + ghosts.shape[0]
    return pl.pallas_call(
        force_kernel,
        out_shape=jax.ShapeDtypeStruct((9, NODE_ROWS, TILE), jnp.float32),
        in_specs=[smem()] * 2 + [vmem()] * 5,
        out_specs=vmem(),
        scratch_shapes=[
            pltpu.VMEM((pool, 6, TILE, TILE), jnp.float32),
            pltpu.VMEM((3, mid.shape[1]), jnp.float32),
        ],
        compiler_params=pltpu.CompilerParams(vmem_limit_bytes=40 << 20),
    )(pairs, counts, mid, line, burgers, node, ghosts)


def returned(grid):
    rows = [passed_along(grid[row], "dx", stride) for stride, row in ((1, 2), (-1, 0))]
    middle = grid[1] + rows[0] + rows[1]
    columns = [passed_along(middle[col], "dy", stride) for stride, col in ((1, 2), (-1, 0))]
    return middle[1] + columns[0] + columns[1]


def on_device(
    seg_mid, seg_line, seg_burgers, seg_cell, seg_node,
    ghost_list, ghost_count, pair_list, pair_count,
):
    mid, line, burgers = seg_mid[0, 0], seg_line[0, 0], seg_burgers[0, 0]
    cells = 8
    seg_data = jnp.concatenate([mid, line, burgers], axis=0)
    own_tiles = seg_data.reshape(9, -1, TILE).transpose(1, 0, 2)
    slots = ghost_list.shape[3]
    packets = own_tiles[ghost_list[0, 0]]
    valid = jnp.arange(slots, dtype=jnp.int32)[None, :] < ghost_count[0, 0][:, None]
    packets = packets * valid.astype(jnp.float32)[:, :, None, None]
    from_left = passed_along(packets[5:8], "dx", 1)
    from_right = passed_along(packets[0:3], "dx", -1)
    upward = jnp.stack([packets[4], from_left[2], from_right[2]])
    downward = jnp.stack([packets[3], from_left[0], from_right[0]])
    from_below = passed_along(upward, "dy", 1)
    from_above = passed_along(downward, "dy", -1)
    groups = [
        from_below[1], from_left[1], from_above[1], from_below[0],
        from_above[0], from_below[2], from_right[1], from_above[2],
    ]
    ghosts = jnp.concatenate(groups, axis=0)
    cell_part = cells_call(mid, line, burgers, seg_cell[0], 9 * cells)
    cell_sum = returned(cell_part.reshape(3, 3, cells, -1))
    moments = cell_sum[:, : 9 * MONO_ROWS].reshape(cells, 9, MONO_ROWS)
    moments = moments[:, :, : len(exponent_rows())].reshape(cells, -1).T
    node_part = force_call(pair_list[0, 0], pair_count[0, 0, :], mid, line, burgers, seg_node[0, 0], ghosts)
    node_sum = returned(node_part.reshape(3, 3, NODE_ROWS, TILE))
    force = node_sum[:12].reshape(3, 4 * TILE)
    return (force[None, None], moments)


def solution(mesh):
    in_specs = (
        P("dx", "dy", None, None),
        P("dx", "dy", None, None),
        P("dx", "dy", None, None),
        P("dx", "dy", None),
        P("dx", "dy", None, None),
        P("dx", "dy", None, None),
        P("dx", "dy", None),
        P("dx", "dy", None, None),
        P("dx", "dy", None),
    )
    out_specs = (P("dx", "dy", None, None), P(None, ("dx", "dy")))
    return jax.shard_map(
        on_device, mesh=mesh, in_specs=in_specs, out_specs=out_specs, check_vma=False
    )
```

```python
import functools

import functools

import jax
import jax.numpy as jnp
from jax import lax
from jax.experimental import pallas as pl
from jax.experimental.pallas import tpu as pltpu
from jax.sharding import PartitionSpec as P

TILE = 128
GROUP = 8
CELL_DEV = 8
MONO_ROWS = 40
NODE_ROWS = 16

core_radius = 0.1
shear_scale = 0.25
neighbour_offsets = ((-1, -1), (-1, 0), (-1, 1), (0, -1), (0, 1), (1, -1), (1, 0), (1, 1))


def exponent_rows():
    rows = []
    for degree in range(5):
        for first in range(degree, -1, -1):
            for second in range(degree - first, -1, -1):
                rows.append((first, second, degree - first - second))
    return rows


def split_two(value):
    high = value.astype(jnp.bfloat16)
    low = (value - high.astype(jnp.float32)).astype(jnp.bfloat16)
    return high, low


def dot_lanes(left, right):
    return lax.dot_general(
        left, right, (((1,), (1,)), ((), ())), preferred_element_type=jnp.float32
    )


def folded(value, span, fold):
    return jnp.where(value >= 6 * span, value - 6 * span, value) if fold else value


def owners(n_dx):
    firsts = (-1, 0) if n_dx == 2 else (-1, 0, 1)
    return [(a, b) for a in firsts for b in (-1, 0, 1)]


def cell_partial(mid_ref, line_ref, burgers_ref, cell_ref, mono_ref, chunk, cells, fold):
    segments = mid_ref.shape[1]
    mono_ref[...] = jnp.zeros_like(mono_ref)
    total = None
    for start in range(0, segments, chunk):
        cols = pl.ds(start, chunk)
        powers = []
        for axis in range(3):
            scaled = 2.0 * (mid_ref[axis : axis + 1, cols] - 0.5)
            square = scaled * scaled
            powers.append((None, scaled, square, square * scaled, square * square))
        for row, exps in enumerate(exponent_rows()):
            value = None
            for axis in range(3):
                if exps[axis]:
                    factor = powers[axis][exps[axis]]
                    value = factor if value is None else value * factor
            if value is None:
                value = jnp.ones((1, chunk), jnp.float32)
            mono_ref[row : row + 1, :] = value
        mono = mono_ref[...]
        highs, lows = [], []
        for beta in range(3):
            b = burgers_ref[beta : beta + 1, cols]
            for gamma in range(3):
                high, low = split_two(mono * (b * line_ref[gamma : gamma + 1, cols]))
                highs.append(high)
                lows.append(low)
        rows = lax.broadcasted_iota(jnp.int32, (TILE, chunk), 0)
        member = jnp.where(rows == folded(cell_ref[0:1, cols], cells, fold), 1.0, 0.0).astype(jnp.bfloat16)
        part = dot_lanes(jnp.concatenate(highs, axis=0), member) + dot_lanes(
            jnp.concatenate(lows, axis=0), member
        )
        total = part if total is None else total + part
    return total


def neighbour(a, b):
    n_dx, n_dy = lax.axis_size("dx"), lax.axis_size("dy")
    i, j = lax.axis_index("dx"), lax.axis_index("dy")
    return (lax.rem(i + (a + n_dx), n_dx), lax.rem(j + (b + n_dy), n_dy))


def greet(offsets):
    barrier = pltpu.get_barrier_semaphore()
    for a, b in offsets:
        pl.semaphore_signal(
            barrier, inc=1, device_id=neighbour(a, b), device_id_type=pl.DeviceIdType.MESH
        )
    return lambda: pl.semaphore_wait(barrier, len(offsets))


def start_copies(offsets, source_of, target_of, send_sem, recv_sem):
    copies = []
    for index, (a, b) in enumerate(offsets):
        copy = pltpu.make_async_remote_copy(
            src_ref=source_of(index),
            dst_ref=target_of(index),
            send_sem=send_sem.at[index],
            recv_sem=recv_sem.at[index],
            device_id=neighbour(a, b),
            device_id_type=pl.DeviceIdType.MESH,
        )
        copy.start()
        copies.append(copy)
    return copies


def cross(burgers, line):
    return [
        burgers[1] * line[2] - burgers[2] * line[1],
        burgers[2] * line[0] - burgers[0] * line[2],
        burgers[0] * line[1] - burgers[1] * line[0],
    ]


def pack_kernel(list_ref, count_ref, mid_ref, line_ref, burgers_ref, packet_ref):
    slots = packet_ref.shape[1]
    for k, offset in enumerate(neighbour_offsets):
        for g in range(slots):
            cols = pl.ds(pl.multiple_of(list_ref[k, g] * TILE, TILE), TILE)
            valid = jnp.where(g < count_ref[k], 1.0, 0.0)
            mid = rows_of(mid_ref, cols)
            mid = [valid * mid[0] - float(offset[0]), valid * mid[1] - float(offset[1]), valid * mid[2]]
            rows = [valid * row for row in rows_of(burgers_ref, cols)]
            moment = cross(rows, [valid * row for row in rows_of(line_ref, cols)])
            rows = mid + [shear_scale * row for row in moment]
            for r, row in enumerate(rows):
                packet_ref[k, g, r : r + 1, :] = row
            packet_ref[k, g, 6:8, :] = jnp.zeros((2, TILE), jnp.float32)


def ghost_kernel(
    cells, fold, packet_ref, mid_ref, line_ref, burgers_ref, cell_ref,
    ghost_ref, out_ref, mono_ref, packed_ref, send_sem, recv_sem,
):
    greet(neighbour_offsets)()
    copies = start_copies(
        neighbour_offsets, lambda k: packet_ref.at[k], lambda k: ghost_ref.at[7 - k],
        send_sem, recv_sem,
    )
    total = cell_partial(
        mid_ref, line_ref, burgers_ref, cell_ref, mono_ref, mono_ref.shape[1], cells, fold
    )
    kept = len(exponent_rows())
    packed_ref[9 * kept :, :] = jnp.zeros((packed_ref.shape[0] - 9 * kept, TILE), jnp.float32)
    for k in range(9):
        packed_ref[k * kept : (k + 1) * kept, :] = total[k * MONO_ROWS : k * MONO_ROWS + kept]
    turned = packed_ref[...].T
    blocks, wide = out_ref.shape[0], out_ref.shape[1] // cells
    for block in range(blocks):
        for part in range(wide):
            out_ref[block, part * cells : (part + 1) * cells, :] = turned[
                block * cells : (block + 1) * cells, part * TILE : (part + 1) * TILE
            ]
    for copy in copies:
        copy.wait()


def return_kernel(part_ref, force_ref, moment_ref, held_ref, turn_ref, send_sem, recv_sem):
    offsets = owners(lax.axis_size("dx"))
    home = offsets.index((0, 0))
    away = [n for n in range(len(offsets)) if n != home]
    greeted = [offsets[n] for n in away]
    greet(greeted)()
    copies = start_copies(
        greeted, lambda n: part_ref.at[away[n]], lambda n: held_ref.at[n], send_sem, recv_sem
    )
    total = part_ref[home]
    for n, copy in enumerate(copies):
        copy.wait()
        total = total + held_ref[n]
    for m in range(3):
        for q in range(4):
            row = 4 * m + q
            force_ref[m : m + 1, q * TILE : (q + 1) * TILE] = total[row : row + 1]
    cells = moment_ref.shape[1]
    wide = (total.shape[0] - NODE_ROWS) // cells
    for part in range(wide):
        first = NODE_ROWS + part * cells
        turn_ref[part * TILE : (part + 1) * TILE, :] = total[first : first + cells].T
    moment_ref[...] = turn_ref[: moment_ref.shape[0], :]


def spread(rows, source_ref, index):
    columns = rows.T
    for q in range(6):
        source_ref[index, q] = jnp.broadcast_to(columns[:, q : q + 1], (TILE, TILE))


def rows_of(ref, cols):
    return [ref[axis : axis + 1, cols] for axis in range(3)]


def force_kernel(
    fold, list_ref, count_ref, mid_ref, line_ref, burgers_ref, node_ref, ghost_ref, cell_ref,
    out_ref, source_ref, force_ref,
):
    own_count = mid_ref.shape[1] // TILE
    slots = ghost_ref.shape[1]

    def spread_own(tile, carry):
        cols = pl.ds(pl.multiple_of(tile * TILE, TILE), TILE)
        moment = cross(rows_of(burgers_ref, cols), rows_of(line_ref, cols))
        rows = rows_of(mid_ref, cols) + [shear_scale * row for row in moment]
        rows = rows + [jnp.zeros((2, TILE), jnp.float32)]
        spread(jnp.concatenate(rows, axis=0), source_ref, tile)
        return carry

    lax.fori_loop(0, own_count, spread_own, 0, unroll=4)

    def spread_ghost(group, carry):
        for slot in range(slots):
            spread(ghost_ref[group, slot], source_ref, own_count + group * slots + slot)
        return carry

    lax.fori_loop(0, 8, spread_ghost, 0, unroll=2)

    def one_tile(tile, carry):
        cols = pl.ds(pl.multiple_of(tile * TILE, TILE), TILE)
        x = [jnp.broadcast_to(row, (GROUP, TILE)) for row in rows_of(mid_ref, cols)]

        def one_slot(slot, sums):
            source = list_ref[tile, slot]
            sums = list(sums)
            for k in range(TILE // GROUP):
                part = pl.ds(k * GROUP, GROUP)
                R = [x[m] - source_ref[source, m, part, :] for m in range(3)]
                g = [source_ref[source, 3 + m, part, :] for m in range(3)]
                r2 = (R[0] * R[0] + core_radius**2) + (R[1] * R[1] + R[2] * R[2])
                inverse = lax.rsqrt(r2)
                inverse2 = inverse * inverse
                weight = inverse2 * inverse
                p = R[0] * g[0] + R[1] * g[1] + R[2] * g[2]
                h = p * (1.5 * inverse2)
                a = [g[m] - h * R[m] for m in range(3)]
                A = [weight * R[m] for m in range(3)]
                sums[0] = sums[0] + A[0] * a[0]
                sums[1] = sums[1] + A[1] * a[1]
                sums[2] = sums[2] + A[2] * a[2]
                sums[3] = sums[3] + (A[0] * a[1] + A[1] * a[0])
                sums[4] = sums[4] + (A[0] * a[2] + A[2] * a[0])
                sums[5] = sums[5] + (A[1] * a[2] + A[2] * a[1])
                sums[6] = sums[6] + weight * p
            return tuple(sums)

        zero = jnp.zeros((GROUP, TILE), jnp.float32)
        sums = lax.fori_loop(0, count_ref[tile], one_slot, (zero,) * 7)
        s = [jnp.sum(value, axis=0, keepdims=True) for value in sums]
        diagonal = s[0] + s[1] + s[2] + 1.5 * s[6]
        xx, yy, zz = [2.0 * s[m] + diagonal for m in range(3)]
        xy, xz, yz = s[3:6]
        b = rows_of(burgers_ref, cols)
        l = rows_of(line_ref, cols)
        t = [
            xx * b[0] + xy * b[1] + xz * b[2],
            xy * b[0] + yy * b[1] + yz * b[2],
            xz * b[0] + yz * b[1] + zz * b[2],
        ]
        force_ref[0:1, cols] = 0.5 * (t[1] * l[2] - t[2] * l[1])
        force_ref[1:2, cols] = 0.5 * (t[2] * l[0] - t[0] * l[2])
        force_ref[2:3, cols] = 0.5 * (t[0] * l[1] - t[1] * l[0])
        return carry

    lax.fori_loop(0, own_count, one_tile, 0)

    directions = out_ref.shape[0]
    chunk = 8 * TILE
    quads = NODE_ROWS // 4

    def nodes(step, total):
        cols = pl.ds(pl.multiple_of(step * chunk, chunk), chunk)
        rows = [jnp.broadcast_to(force_ref[m : m + 1, cols], (4, chunk)) for m in range(3)]
        rows = jnp.concatenate(rows + [jnp.zeros((4, chunk), jnp.float32)], axis=0)
        high = rows.astype(jnp.bfloat16).astype(jnp.float32)
        low = rows - high
        place = lax.broadcasted_iota(jnp.int32, (NODE_ROWS, chunk), 0) % quads
        lanes = lax.broadcasted_iota(jnp.int32, (TILE, chunk), 0)
        for end in range(2):
            node = node_ref[end : end + 1, cols]
            member = jnp.where(lanes == node % TILE, 1.0, 0.0).astype(jnp.bfloat16)
            block = folded(node // TILE, quads, fold) - place
            left = []
            for value in (high, low):
                for d in range(directions):
                    chosen = jnp.where(block == d * quads, value, 0.0)
                    left.append(chosen.astype(jnp.bfloat16))
            total = total + dot_lanes(jnp.concatenate(left, axis=0), member)
        return total

    total = lax.fori_loop(
        0, mid_ref.shape[1] // chunk, nodes,
        jnp.zeros((2 * directions * NODE_ROWS, TILE), jnp.float32),
    )
    half = directions * NODE_ROWS
    total = (total[:half] + total[half:]).reshape(directions, NODE_ROWS, TILE)
    out_ref[:, :NODE_ROWS, :] = total
    out_ref[:, NODE_ROWS:, :] = cell_ref[...]


def vmem():
    return pl.BlockSpec(memory_space=pltpu.VMEM)


def smem():
    return pl.BlockSpec(memory_space=pltpu.SMEM)


def pack_call(lists, counts, mid, line, burgers):
    return pl.pallas_call(
        pack_kernel,
        out_shape=jax.ShapeDtypeStruct((8, lists.shape[1], 8, TILE), jnp.float32),
        in_specs=[smem()] * 2 + [vmem()] * 3,
        out_specs=vmem(),
        compiler_params=pltpu.CompilerParams(vmem_limit_bytes=16 << 20),
    )(lists, counts, mid, line, burgers)


def ghost_call(packets, mid, line, burgers, cell, cells, blocks):
    fold = blocks == 6
    slots = packets.shape[1]
    wide = pl.cdiv(9 * len(exponent_rows()), TILE)
    return pl.pallas_call(
        functools.partial(ghost_kernel, cells, fold),
        out_shape=(
            jax.ShapeDtypeStruct((8, slots, 8, TILE), jnp.float32),
            jax.ShapeDtypeStruct((blocks, wide * cells, TILE), jnp.float32),
        ),
        in_specs=[vmem()] * 5,
        out_specs=(vmem(), vmem()),
        scratch_shapes=[
            pltpu.VMEM((MONO_ROWS, 4 * TILE), jnp.float32),
            pltpu.VMEM((wide * TILE, TILE), jnp.float32),
            pltpu.SemaphoreType.DMA((8,)),
            pltpu.SemaphoreType.DMA((8,)),
        ],
        compiler_params=pltpu.CompilerParams(
            collective_id=0, has_side_effects=True, vmem_limit_bytes=16 << 20
        ),
    )(packets, mid, line, burgers, cell)


def force_call(pairs, counts, mid, line, burgers, node, ghosts, cell_part):
    pool = mid.shape[1] // TILE + ghosts.shape[0] * ghosts.shape[1]
    blocks, rows, _ = cell_part.shape
    return pl.pallas_call(
        functools.partial(force_kernel, blocks == 6),
        out_shape=jax.ShapeDtypeStruct((blocks, NODE_ROWS + rows, TILE), jnp.float32),
        in_specs=[smem()] * 2 + [vmem()] * 6,
        out_specs=vmem(),
        scratch_shapes=[
            pltpu.VMEM((pool, 6, TILE, TILE), jnp.float32),
            pltpu.VMEM((3, mid.shape[1]), jnp.float32),
        ],
        compiler_params=pltpu.CompilerParams(vmem_limit_bytes=40 << 20),
    )(pairs, counts, mid, line, burgers, node, ghosts, cell_part)


def return_call(parts, cells):
    blocks, rows, _ = parts.shape
    wide = (rows - NODE_ROWS) // cells
    return pl.pallas_call(
        return_kernel,
        out_shape=(
            jax.ShapeDtypeStruct((3, 4 * TILE), jnp.float32),
            jax.ShapeDtypeStruct((9 * len(exponent_rows()), cells), jnp.float32),
        ),
        in_specs=[vmem()],
        out_specs=(vmem(), vmem()),
        scratch_shapes=[
            pltpu.VMEM((blocks - 1, rows, TILE), jnp.float32),
            pltpu.VMEM((wide * TILE, cells), jnp.float32),
            pltpu.SemaphoreType.DMA((blocks - 1,)),
            pltpu.SemaphoreType.DMA((blocks - 1,)),
        ],
        compiler_params=pltpu.CompilerParams(
            collective_id=1, has_side_effects=True, vmem_limit_bytes=16 << 20
        ),
    )(parts)


def on_device(
    seg_mid, seg_line, seg_burgers, seg_cell, seg_node,
    ghost_list, ghost_count, pair_list, pair_count,
):
    mid, line, burgers = seg_mid[0, 0], seg_line[0, 0], seg_burgers[0, 0]
    cells = CELL_DEV
    blocks = len(owners(lax.axis_size("dx")))
    packets = pack_call(ghost_list[0, 0], ghost_count[0, 0], mid, line, burgers)
    ghosts, cell_part = ghost_call(packets, mid, line, burgers, seg_cell[0], cells, blocks)
    parts = force_call(
        pair_list[0, 0], pair_count[0, 0], mid, line, burgers, seg_node[0, 0], ghosts, cell_part
    )
    force, moments = return_call(parts, cells)
    return (force[None, None], moments)


def solution(mesh):
    in_specs = (
        P("dx", "dy", None, None),
        P("dx", "dy", None, None),
        P("dx", "dy", None, None),
        P("dx", "dy", None),
        P("dx", "dy", None, None),
        P("dx", "dy", None, None),
        P("dx", "dy", None),
        P("dx", "dy", None, None),
        P("dx", "dy", None),
    )
    out_specs = (P("dx", "dy", None, None), P(None, ("dx", "dy")))
    return jax.shard_map(
        on_device, mesh=mesh, in_specs=in_specs, out_specs=out_specs, check_vma=False
    )
```

```python
import functools

import functools

import jax
import jax.numpy as jnp
from jax import lax
from jax.experimental import pallas as pl
from jax.experimental.pallas import tpu as pltpu
from jax.sharding import PartitionSpec as P

TILE = 128
GROUP = 8
CELL_DEV = 8
MONO_ROWS = 40
NODE_ROWS = 16

core_radius = 0.1
shear_scale = 0.25
neighbour_offsets = ((-1, -1), (-1, 0), (-1, 1), (0, -1), (0, 1), (1, -1), (1, 0), (1, 1))


def exponent_rows():
    rows = []
    for degree in range(5):
        for first in range(degree, -1, -1):
            for second in range(degree - first, -1, -1):
                rows.append((first, second, degree - first - second))
    return rows


def split_two(value):
    high = value.astype(jnp.bfloat16)
    low = (value - high.astype(jnp.float32)).astype(jnp.bfloat16)
    return high, low


def dot_lanes(left, right):
    return lax.dot_general(
        left, right, (((1,), (1,)), ((), ())), preferred_element_type=jnp.float32
    )


def folded(value, span, fold):
    return jnp.where(value >= 6 * span, value - 6 * span, value) if fold else value


def owners(n_dx):
    firsts = (-1, 0) if n_dx == 2 else (-1, 0, 1)
    return [(a, b) for a in firsts for b in (-1, 0, 1)]


def cell_partial(mid_ref, line_ref, burgers_ref, cell_ref, mono_ref, chunk, cells, fold):
    segments = mid_ref.shape[1]
    mono_ref[...] = jnp.zeros_like(mono_ref)
    total = None
    for start in range(0, segments, chunk):
        cols = pl.ds(start, chunk)
        powers = []
        for axis in range(3):
            scaled = 2.0 * (mid_ref[axis : axis + 1, cols] - 0.5)
            square = scaled * scaled
            powers.append((None, scaled, square, square * scaled, square * square))
        for row, exps in enumerate(exponent_rows()):
            value = None
            for axis in range(3):
                if exps[axis]:
                    factor = powers[axis][exps[axis]]
                    value = factor if value is None else value * factor
            if value is None:
                value = jnp.ones((1, chunk), jnp.float32)
            mono_ref[row : row + 1, :] = value
        mono = mono_ref[...]
        highs, lows = [], []
        for beta in range(3):
            b = burgers_ref[beta : beta + 1, cols]
            for gamma in range(3):
                high, low = split_two(mono * (b * line_ref[gamma : gamma + 1, cols]))
                highs.append(high)
                lows.append(low)
        rows = lax.broadcasted_iota(jnp.int32, (TILE, chunk), 0)
        member = jnp.where(rows == folded(cell_ref[0:1, cols], cells, fold), 1.0, 0.0).astype(jnp.bfloat16)
        part = dot_lanes(jnp.concatenate(highs, axis=0), member) + dot_lanes(
            jnp.concatenate(lows, axis=0), member
        )
        total = part if total is None else total + part
    return total


def neighbour(a, b):
    n_dx, n_dy = lax.axis_size("dx"), lax.axis_size("dy")
    i, j = lax.axis_index("dx"), lax.axis_index("dy")
    return (lax.rem(i + (a + n_dx), n_dx), lax.rem(j + (b + n_dy), n_dy))


def greet(offsets):
    barrier = pltpu.get_barrier_semaphore()
    for a, b in offsets:
        pl.semaphore_signal(
            barrier, inc=1, device_id=neighbour(a, b), device_id_type=pl.DeviceIdType.MESH
        )
    return lambda: pl.semaphore_wait(barrier, len(offsets))


def start_copies(offsets, source_of, target_of, send_sem, recv_sem):
    copies = []
    for index, (a, b) in enumerate(offsets):
        copy = pltpu.make_async_remote_copy(
            src_ref=source_of(index),
            dst_ref=target_of(index),
            send_sem=send_sem.at[index],
            recv_sem=recv_sem.at[index],
            device_id=neighbour(a, b),
            device_id_type=pl.DeviceIdType.MESH,
        )
        copy.start()
        copies.append(copy)
    return copies


def cross(burgers, line):
    return [
        burgers[1] * line[2] - burgers[2] * line[1],
        burgers[2] * line[0] - burgers[0] * line[2],
        burgers[0] * line[1] - burgers[1] * line[0],
    ]


def pack_kernel(list_ref, count_ref, mid_ref, line_ref, burgers_ref, packet_ref):
    slots = packet_ref.shape[1]
    for k, offset in enumerate(neighbour_offsets):
        for g in range(slots):
            cols = pl.ds(pl.multiple_of(list_ref[k, g] * TILE, TILE), TILE)
            valid = jnp.where(g < count_ref[k], 1.0, 0.0)
            mid = rows_of(mid_ref, cols)
            mid = [valid * mid[0] - float(offset[0]), valid * mid[1] - float(offset[1]), valid * mid[2]]
            rows = [valid * row for row in rows_of(burgers_ref, cols)]
            moment = cross(rows, [valid * row for row in rows_of(line_ref, cols)])
            rows = mid + [shear_scale * row for row in moment]
            for r, row in enumerate(rows):
                packet_ref[k, g, r : r + 1, :] = row
            packet_ref[k, g, 6:8, :] = jnp.zeros((2, TILE), jnp.float32)


def ghost_kernel(
    cells, fold, packet_ref, mid_ref, line_ref, burgers_ref, cell_ref,
    ghost_ref, out_ref, mono_ref, packed_ref, send_sem, recv_sem,
):
    greet(neighbour_offsets)()
    copies = start_copies(
        neighbour_offsets, lambda k: packet_ref.at[k], lambda k: ghost_ref.at[7 - k],
        send_sem, recv_sem,
    )
    total = cell_partial(
        mid_ref, line_ref, burgers_ref, cell_ref, mono_ref, mono_ref.shape[1], cells, fold
    )
    kept = len(exponent_rows())
    packed_ref[9 * kept :, :] = jnp.zeros((packed_ref.shape[0] - 9 * kept, TILE), jnp.float32)
    for k in range(9):
        packed_ref[k * kept : (k + 1) * kept, :] = total[k * MONO_ROWS : k * MONO_ROWS + kept]
    turned = packed_ref[...].T
    blocks, wide = out_ref.shape[0], out_ref.shape[1] // cells
    for block in range(blocks):
        for part in range(wide):
            out_ref[block, part * cells : (part + 1) * cells, :] = turned[
                block * cells : (block + 1) * cells, part * TILE : (part + 1) * TILE
            ]
    for copy in copies:
        copy.wait()


def return_kernel(part_ref, force_ref, moment_ref, held_ref, turn_ref, send_sem, recv_sem):
    offsets = owners(lax.axis_size("dx"))
    home = offsets.index((0, 0))
    away = [n for n in range(len(offsets)) if n != home]
    greeted = [offsets[n] for n in away]
    greet(greeted)()
    copies = start_copies(
        greeted, lambda n: part_ref.at[away[n]], lambda n: held_ref.at[n], send_sem, recv_sem
    )
    total = part_ref[home]
    for n, copy in enumerate(copies):
        copy.wait()
        total = total + held_ref[n]
    for m in range(3):
        for q in range(4):
            row = 4 * m + q
            force_ref[m : m + 1, q * TILE : (q + 1) * TILE] = total[row : row + 1]
    cells = moment_ref.shape[1]
    wide = (total.shape[0] - NODE_ROWS) // cells
    for part in range(wide):
        first = NODE_ROWS + part * cells
        turn_ref[part * TILE : (part + 1) * TILE, :] = total[first : first + cells].T
    moment_ref[...] = turn_ref[: moment_ref.shape[0], :]


def spread(rows, source_ref, index):
    high = rows.astype(jnp.bfloat16).astype(jnp.float32)
    rest = rows - high
    middle = rest.astype(jnp.bfloat16).astype(jnp.float32)
    pieces = jnp.concatenate([high, middle, rest - middle], axis=0).astype(jnp.bfloat16)
    shape = (pieces.shape[0], 6 * TILE)
    piece_row = lax.broadcasted_iota(jnp.int32, shape, 0) % GROUP
    column = lax.broadcasted_iota(jnp.int32, shape, 1) // TILE
    select = jnp.where(piece_row == column, 1.0, 0.0).astype(jnp.bfloat16)
    wide = lax.dot_general(
        pieces, select, (((0,), (0,)), ((), ())), preferred_element_type=jnp.float32
    )
    for q in range(6):
        source_ref[index, q] = wide[:, q * TILE : (q + 1) * TILE]


def rows_of(ref, cols):
    return [ref[axis : axis + 1, cols] for axis in range(3)]


def force_kernel(
    fold, list_ref, count_ref, mid_ref, line_ref, burgers_ref, node_ref, ghost_ref, cell_ref,
    out_ref, source_ref, force_ref,
):
    own_count = mid_ref.shape[1] // TILE
    slots = ghost_ref.shape[1]

    def spread_own(tile, carry):
        cols = pl.ds(pl.multiple_of(tile * TILE, TILE), TILE)
        moment = cross(rows_of(burgers_ref, cols), rows_of(line_ref, cols))
        rows = rows_of(mid_ref, cols) + [shear_scale * row for row in moment]
        rows = rows + [jnp.zeros((2, TILE), jnp.float32)]
        spread(jnp.concatenate(rows, axis=0), source_ref, tile)
        return carry

    lax.fori_loop(0, own_count, spread_own, 0, unroll=4)

    def spread_ghost(group, carry):
        for slot in range(slots):
            spread(ghost_ref[group, slot], source_ref, own_count + group * slots + slot)
        return carry

    lax.fori_loop(0, 8, spread_ghost, 0, unroll=2)

    def one_tile(tile, carry):
        cols = pl.ds(pl.multiple_of(tile * TILE, TILE), TILE)
        x = [jnp.broadcast_to(row, (GROUP, TILE)) for row in rows_of(mid_ref, cols)]

        def one_slot(slot, sums):
            source = list_ref[tile, slot]
            sums = list(sums)
            for k in range(TILE // GROUP):
                part = pl.ds(k * GROUP, GROUP)
                R = [x[m] - source_ref[source, m, part, :] for m in range(3)]
                g = [source_ref[source, 3 + m, part, :] for m in range(3)]
                r2 = (R[0] * R[0] + core_radius**2) + (R[1] * R[1] + R[2] * R[2])
                inverse = lax.rsqrt(r2)
                inverse2 = inverse * inverse
                weight = inverse2 * inverse
                p = R[0] * g[0] + R[1] * g[1] + R[2] * g[2]
                h = p * (1.5 * inverse2)
                a = [g[m] - h * R[m] for m in range(3)]
                A = [weight * R[m] for m in range(3)]
                sums[0] = sums[0] + A[0] * a[0]
                sums[1] = sums[1] + A[1] * a[1]
                sums[2] = sums[2] + A[2] * a[2]
                sums[3] = sums[3] + (A[0] * a[1] + A[1] * a[0])
                sums[4] = sums[4] + (A[0] * a[2] + A[2] * a[0])
                sums[5] = sums[5] + (A[1] * a[2] + A[2] * a[1])
                sums[6] = sums[6] + weight * p
            return tuple(sums)

        zero = jnp.zeros((GROUP, TILE), jnp.float32)
        sums = lax.fori_loop(0, count_ref[tile], one_slot, (zero,) * 7)
        s = [jnp.sum(value, axis=0, keepdims=True) for value in sums]
        diagonal = s[0] + s[1] + s[2] + 1.5 * s[6]
        xx, yy, zz = [2.0 * s[m] + diagonal for m in range(3)]
        xy, xz, yz = s[3:6]
        b = rows_of(burgers_ref, cols)
        l = rows_of(line_ref, cols)
        t = [
            xx * b[0] + xy * b[1] + xz * b[2],
            xy * b[0] + yy * b[1] + yz * b[2],
            xz * b[0] + yz * b[1] + zz * b[2],
        ]
        force_ref[0:1, cols] = 0.5 * (t[1] * l[2] - t[2] * l[1])
        force_ref[1:2, cols] = 0.5 * (t[2] * l[0] - t[0] * l[2])
        force_ref[2:3, cols] = 0.5 * (t[0] * l[1] - t[1] * l[0])
        return carry

    lax.fori_loop(0, own_count, one_tile, 0)

    directions = out_ref.shape[0]
    chunk = 8 * TILE
    quads = NODE_ROWS // 4

    def nodes(step, total):
        cols = pl.ds(pl.multiple_of(step * chunk, chunk), chunk)
        rows = [jnp.broadcast_to(force_ref[m : m + 1, cols], (4, chunk)) for m in range(3)]
        rows = jnp.concatenate(rows + [jnp.zeros((4, chunk), jnp.float32)], axis=0)
        high = rows.astype(jnp.bfloat16).astype(jnp.float32)
        low = rows - high
        place = lax.broadcasted_iota(jnp.int32, (NODE_ROWS, chunk), 0) % quads
        lanes = lax.broadcasted_iota(jnp.int32, (TILE, chunk), 0)
        for end in range(2):
            node = node_ref[end : end + 1, cols]
            member = jnp.where(lanes == node % TILE, 1.0, 0.0).astype(jnp.bfloat16)
            block = folded(node // TILE, quads, fold) - place
            left = []
            for value in (high, low):
                for d in range(directions):
                    chosen = jnp.where(block == d * quads, value, 0.0)
                    left.append(chosen.astype(jnp.bfloat16))
            total = total + dot_lanes(jnp.concatenate(left, axis=0), member)
        return total

    total = lax.fori_loop(
        0, mid_ref.shape[1] // chunk, nodes,
        jnp.zeros((2 * directions * NODE_ROWS, TILE), jnp.float32),
    )
    half = directions * NODE_ROWS
    total = (total[:half] + total[half:]).reshape(directions, NODE_ROWS, TILE)
    out_ref[:, :NODE_ROWS, :] = total
    out_ref[:, NODE_ROWS:, :] = cell_ref[...]


def vmem():
    return pl.BlockSpec(memory_space=pltpu.VMEM)


def smem():
    return pl.BlockSpec(memory_space=pltpu.SMEM)


def pack_call(lists, counts, mid, line, burgers):
    return pl.pallas_call(
        pack_kernel,
        out_shape=jax.ShapeDtypeStruct((8, lists.shape[1], 8, TILE), jnp.float32),
        in_specs=[smem()] * 2 + [vmem()] * 3,
        out_specs=vmem(),
        compiler_params=pltpu.CompilerParams(vmem_limit_bytes=16 << 20),
    )(lists, counts, mid, line, burgers)


def ghost_call(packets, mid, line, burgers, cell, cells, blocks):
    fold = blocks == 6
    slots = packets.shape[1]
    wide = pl.cdiv(9 * len(exponent_rows()), TILE)
    return pl.pallas_call(
        functools.partial(ghost_kernel, cells, fold),
        out_shape=(
            jax.ShapeDtypeStruct((8, slots, 8, TILE), jnp.float32),
            jax.ShapeDtypeStruct((blocks, wide * cells, TILE), jnp.float32),
        ),
        in_specs=[vmem()] * 5,
        out_specs=(vmem(), vmem()),
        scratch_shapes=[
            pltpu.VMEM((MONO_ROWS, 4 * TILE), jnp.float32),
            pltpu.VMEM((wide * TILE, TILE), jnp.float32),
            pltpu.SemaphoreType.DMA((8,)),
            pltpu.SemaphoreType.DMA((8,)),
        ],
        compiler_params=pltpu.CompilerParams(
            collective_id=0, has_side_effects=True, vmem_limit_bytes=16 << 20
        ),
    )(packets, mid, line, burgers, cell)


def force_call(pairs, counts, mid, line, burgers, node, ghosts, cell_part):
    pool = mid.shape[1] // TILE + ghosts.shape[0] * ghosts.shape[1]
    blocks, rows, _ = cell_part.shape
    return pl.pallas_call(
        functools.partial(force_kernel, blocks == 6),
        out_shape=jax.ShapeDtypeStruct((blocks, NODE_ROWS + rows, TILE), jnp.float32),
        in_specs=[smem()] * 2 + [vmem()] * 6,
        out_specs=vmem(),
        scratch_shapes=[
            pltpu.VMEM((pool, 6, TILE, TILE), jnp.float32),
            pltpu.VMEM((3, mid.shape[1]), jnp.float32),
        ],
        compiler_params=pltpu.CompilerParams(vmem_limit_bytes=40 << 20),
    )(pairs, counts, mid, line, burgers, node, ghosts, cell_part)


def return_call(parts, cells):
    blocks, rows, _ = parts.shape
    wide = (rows - NODE_ROWS) // cells
    return pl.pallas_call(
        return_kernel,
        out_shape=(
            jax.ShapeDtypeStruct((3, 4 * TILE), jnp.float32),
            jax.ShapeDtypeStruct((9 * len(exponent_rows()), cells), jnp.float32),
        ),
        in_specs=[vmem()],
        out_specs=(vmem(), vmem()),
        scratch_shapes=[
            pltpu.VMEM((blocks - 1, rows, TILE), jnp.float32),
            pltpu.VMEM((wide * TILE, cells), jnp.float32),
            pltpu.SemaphoreType.DMA((blocks - 1,)),
            pltpu.SemaphoreType.DMA((blocks - 1,)),
        ],
        compiler_params=pltpu.CompilerParams(
            collective_id=1, has_side_effects=True, vmem_limit_bytes=16 << 20
        ),
    )(parts)


def on_device(
    seg_mid, seg_line, seg_burgers, seg_cell, seg_node,
    ghost_list, ghost_count, pair_list, pair_count,
):
    mid, line, burgers = seg_mid[0, 0], seg_line[0, 0], seg_burgers[0, 0]
    cells = CELL_DEV
    blocks = len(owners(lax.axis_size("dx")))
    packets = pack_call(ghost_list[0, 0], ghost_count[0, 0], mid, line, burgers)
    ghosts, cell_part = ghost_call(packets, mid, line, burgers, seg_cell[0], cells, blocks)
    parts = force_call(
        pair_list[0, 0], pair_count[0, 0], mid, line, burgers, seg_node[0, 0], ghosts, cell_part
    )
    force, moments = return_call(parts, cells)
    return (force[None, None], moments)


def solution(mesh):
    in_specs = (
        P("dx", "dy", None, None),
        P("dx", "dy", None, None),
        P("dx", "dy", None, None),
        P("dx", "dy", None),
        P("dx", "dy", None, None),
        P("dx", "dy", None, None),
        P("dx", "dy", None),
        P("dx", "dy", None, None),
        P("dx", "dy", None),
    )
    out_specs = (P("dx", "dy", None, None), P(None, ("dx", "dy")))
    return jax.shard_map(
        on_device, mesh=mesh, in_specs=in_specs, out_specs=out_specs, check_vma=False
    )
```
